32 devices in a mesh: ctx: 8 (over y, x, core), dp: 4 (over z).
Axes of the slice: x: 2, y: 2, z: 4, core: 2. Of those that a mesh axis runs over, the one named last changes fastest.
Arguments:
- tokens: bfloat16 [4, 1024, 768], P('dp', 'ctx'), may hold values from -6 to 6
- cotangent: bfloat16 [4, 1024, 768], P('dp', 'ctx'), may hold values from -6 to 6
- qkv_weight: float32 [768, 2304], P(('ctx', 'dp')), may hold values from -0.21875 to 0.21875
- attn_out_weight: float32 [768, 768], P(('ctx', 'dp')), may hold values from -6 to 6
- mlp_in_weight: float32 [768, 2304], P(('ctx', 'dp')), may hold values from -0.21875 to 0.21875
- mlp_out_weight: float32 [1152, 768], P(None, ('ctx', 'dp')), may hold values from -0.1875 to 0.1875
- attn_gain: float32 [768], P(('ctx', 'dp')), may hold values from 0.5 to 1.5
- mlp_gain: float32 [768], P(('ctx', 'dp')), may hold values from 0.5 to 1.5
Outputs:
- output: bfloat16 [4, 1024, 768], P('dp', 'ctx')
- tokens_grad: bfloat16 [4, 1024, 768], P('dp', 'ctx')
- qkv_grad: float32 [768, 2304], P(('ctx', 'dp'))
- attn_out_grad: float32 [768, 768], P(('ctx', 'dp'))
- mlp_in_grad: float32 [768, 2304], P(('ctx', 'dp'))
- mlp_out_grad: float32 [1152, 768], P(None, ('ctx', 'dp'))
- attn_gain_grad: float32 [768], P(('ctx', 'dp'))
- mlp_gain_grad: float32 [768], P(('ctx', 'dp'))
The draws below stay inside these ranges and needn't reach their ends.
All inputs are finite; a program needn't handle non-finite values.
Results may differ from the reference program's by a relative error of at most 0.02.
Values may be sent and summed in bfloat16 or wider, within the bound.
A program may use at most 320 MiB of HBM per device.

```python
from functools import partial
import jax
import jax.numpy as jnp
from jax import lax

D = 768
HEADS = 12
FF = 1152
LEN = 1024
ROWS = 4


def block_levels(rng, extent, cuts, least, top_value):
    level, own = 1.0, jax.random.fold_in(rng, 6)
    for position, blocks in cuts:
        heights = jnp.exp(jax.random.uniform(jax.random.fold_in(own, position), (blocks,), jnp.float32, least / len(cuts), top_value / len(cuts)))
        level = level * jnp.repeat(heights, extent[position] // blocks).reshape([-1 if axis == position else 1 for axis in range(len(extent))])
    return level


def normal_values(own_key, extent, deviation, bound, split=(), kind=jnp.bfloat16):
    factor_of = block_levels(own_key, extent, split, -0.22, 0.18) if split else 1.0
    array = jax.random.normal(own_key, extent, jnp.float32) * deviation * factor_of
    return jnp.minimum(jnp.maximum(array, -bound), bound).astype(kind)


def setup_inputs(seed: int = 0) -> dict:
    splits = jax.random.split(jax.random.key(seed), 9)
    tokens = normal_values(splits[0], (ROWS, LEN, D), 1.0, 6.0, ((0, 4), (1, 8)))
    cotangent = normal_values(splits[1], (ROWS, LEN, D), 1.0, 6.0, ((0, 4), (1, 8)))
    qkv_weight = normal_values(splits[2], (D, 3 * D), D ** -0.5, 0.21875, ((0, 32),), jnp.float32)
    attn_out_weight = normal_values(splits[3], (D, D), (LEN ** 0.5 * (3 * D) ** -0.5), 6.0, ((0, 32),), jnp.float32)
    mlp_in_weight = normal_values(splits[4], (D, 2 * FF), D ** -0.5, 0.21875, ((0, 32),), jnp.float32)
    mlp_out_weight = normal_values(splits[5], (FF, D), FF ** -0.5, 0.1875, ((1, 32),), jnp.float32)
    attn_gain = jnp.clip(1.0 + 0.1 * jax.random.normal(splits[6], (D,), jnp.float32), 0.5, 1.5)
    mlp_gain = jnp.clip(1.0 + 0.1 * jax.random.normal(splits[7], (D,), jnp.float32), 0.5, 1.5)
    return {"tokens": tokens, "cotangent": cotangent, "qkv_weight": qkv_weight, "attn_out_weight": attn_out_weight, "mlp_in_weight": mlp_in_weight, "mlp_out_weight": mlp_out_weight, "attn_gain": attn_gain, "mlp_gain": mlp_gain}


@jax.custom_vjp
def low(v):
    return lax.optimization_barrier(v.astype(jnp.bfloat16)).astype(jnp.float32)

@jax.custom_vjp
def low_back(v):
    return v

def low_keep(v):
    return (low(v), None)

def low_pass(kept, grad):
    return (grad,)

def back_keep(v):
    return (v, None)

def back_low(kept, grad):
    return (low(grad),)
low.defvjp(low_keep, low_pass)
low_back.defvjp(back_keep, back_low)
eps_norm = 1e-05
theta_base = 160000.0
highest = lax.Precision.HIGHEST

def norm_rows(values, scaling):
    center = values - lax.optimization_barrier(jnp.mean(values, axis=-1, keepdims=True))
    spread = lax.optimization_barrier(jnp.mean(center * center, axis=-1, keepdims=True))
    return center * lax.rsqrt(spread + eps_norm) * scaling

def turn_tables(offset, length, head_size):
    halfway = head_size // 2
    inverse = theta_base ** (-(jnp.arange(halfway, dtype=jnp.float32) * 2.0 / head_size))
    places = (offset + jnp.arange(length, dtype=jnp.int32)).astype(jnp.float32)
    angles = places[:, None] * inverse[None, :]
    cosine = jnp.concatenate([jnp.cos(angles), jnp.cos(angles)], axis=-1)[:, None, :]
    sine_table = jnp.concatenate([jnp.sin(angles), jnp.sin(angles)], axis=-1)[:, None, :]
    return (cosine, sine_table)

def rotate(values, cosine, sine_table):
    halfway = values.shape[-1] // 2
    turned = jnp.concatenate([-values[..., halfway:], values[..., :halfway]], axis=-1)
    return values * cosine + turned * sine_table

def attend_block(query_block, keys_in, values_in):
    factor = keys_in.shape[-1] ** (-0.5)
    scores = low_back(jnp.einsum('qhd,khd->hqk', query_block, keys_in, precision=highest) * factor)
    summit = lax.optimization_barrier(jnp.max(scores, axis=-1, keepdims=True))
    chances = jnp.exp(scores - summit)
    chances = low(chances / lax.optimization_barrier(jnp.sum(chances, axis=-1, keepdims=True)))
    return jnp.einsum('hqk,khd->qhd', chances, values_in, precision=highest)

def layer_rows(inputs, weights):
    w_qkv, w_attn, w_inner, w_outer, gain_attn, gain_mlp = weights
    length, breadth = inputs.shape
    head_count = HEADS
    head_size = breadth // head_count
    normed = low(norm_rows(inputs, gain_attn))
    projected = low_back(jnp.dot(normed, w_qkv, precision=highest))
    cosine, sine_table = turn_tables(0, length, head_size)
    queries = low(rotate(projected[:, :breadth].reshape(length, head_count, head_size), cosine, sine_table))
    keys_in = low(rotate(projected[:, breadth:2 * breadth].reshape(length, head_count, head_size), cosine, sine_table))
    values_in = low(projected[:, 2 * breadth:].reshape(length, head_count, head_size))
    block_rows = min(512, length)
    blocks = queries.reshape(length // block_rows, block_rows, head_count, head_size)
    attended = lax.map(jax.checkpoint(partial(attend_block, keys_in=keys_in, values_in=values_in)), blocks)
    attended = low(low_back(attended.reshape(length, breadth)))
    branch = low_back(jnp.dot(attended, w_attn, precision=highest))
    middle = inputs + branch
    normed_mlp = low(norm_rows(middle, gain_mlp))
    widened = low_back(jnp.dot(normed_mlp, w_inner, precision=highest))
    hidden_half = widened.shape[-1] // 2
    gated_units = low(jax.nn.gelu(widened[:, :hidden_half], approximate=False) * widened[:, hidden_half:])
    return middle + low_back(jnp.dot(gated_units, w_outer, precision=highest))

def forward(inputs, weights):
    rounded = tuple((low(member) for member in weights))

    def advance(carried, document):
        return (carried, layer_rows(document, rounded))
    unused, outputs = lax.scan(advance, jnp.zeros((), jnp.float32), inputs)
    return outputs

def reference(tokens, cotangent, qkv_weight, attn_out_weight, mlp_in_weight, mlp_out_weight, attn_gain, mlp_gain):
    weights = (qkv_weight, attn_out_weight, mlp_in_weight, mlp_out_weight, attn_gain, mlp_gain)
    outputs, pull_back = jax.vjp(forward, tokens.astype(jnp.float32), weights)
    input_grad, weight_grads = pull_back(cotangent.astype(jnp.float32))
    return (outputs.astype(jnp.bfloat16), input_grad.astype(jnp.bfloat16), weight_grads[0], weight_grads[1], weight_grads[2], weight_grads[3], weight_grads[4], weight_grads[5])
```

```python
import jax
import jax.numpy as jnp
import numpy as np
from jax import lax
from jax.experimental import pallas as pl
from jax.experimental.pallas import tpu as pltpu
from jax.sharding import PartitionSpec as P

HEADS = 12


eps_norm = 1e-05
theta_base = 160000.0


def norm_rows(values, scaling):
    center = values - jnp.mean(values, axis=-1, keepdims=True)
    spread = jnp.mean(center * center, axis=-1, keepdims=True)
    return center * lax.rsqrt(spread + eps_norm) * scaling


def turn_tables(offset, length, head_size):
    halfway = head_size // 2
    inverse = theta_base ** (-(jnp.arange(halfway, dtype=jnp.float32) * 2.0 / head_size))
    places = (offset + jnp.arange(length, dtype=jnp.int32)).astype(jnp.float32)
    angles = places[:, None] * inverse[None, :]
    cosine = jnp.concatenate([jnp.cos(angles), jnp.cos(angles)], axis=-1)[:, None, :]
    sine_table = jnp.concatenate([jnp.sin(angles), jnp.sin(angles)], axis=-1)[:, None, :]
    return (cosine, sine_table)


def rotate(values, cosine, sine_table):
    halfway = values.shape[-1] // 2
    turned = jnp.concatenate([-values[..., halfway:], values[..., :halfway]], axis=-1)
    return values * cosine + turned * sine_table


def glu_units(widened):
    hidden_half = widened.shape[-1] // 2
    return jax.nn.gelu(widened[..., :hidden_half], approximate=False) * widened[..., hidden_half:]


def split_heads(values, head_count):
    return values.reshape(
        values.shape[0], values.shape[1], head_count, values.shape[2] // head_count
    )


def body(
    tokens,
    cotangent,
    qkv_weight,
    attn_out_weight,
    mlp_in_weight,
    mlp_out_weight,
    attn_gain,
    mlp_gain,
):
    seq_count, local_rows, breadth = tokens.shape
    head_count = HEADS
    head_size = breadth // head_count
    factor = head_size ** (-0.5)
    flat_rows = seq_count * local_rows
    shards = (
        qkv_weight.astype(jnp.bfloat16),
        attn_out_weight.astype(jnp.bfloat16),
        mlp_in_weight.astype(jnp.bfloat16),
        mlp_out_weight.astype(jnp.bfloat16),
        attn_gain.astype(jnp.bfloat16),
        mlp_gain.astype(jnp.bfloat16),
    )
    whole = (
        lax.all_gather(shards[0], ("ctx", "dp"), axis=0, tiled=True),
        lax.all_gather(shards[1], ("ctx", "dp"), axis=0, tiled=True),
        lax.all_gather(shards[2], ("ctx", "dp"), axis=0, tiled=True),
        lax.all_gather(shards[3], ("ctx", "dp"), axis=1, tiled=True),
        lax.all_gather(shards[4], ("ctx", "dp"), axis=0, tiled=True),
        lax.all_gather(shards[5], ("ctx", "dp"), axis=0, tiled=True),
    )
    w_qkv, w_attn, w_inner, w_outer, gain_low_attn, gain_low_mlp = whole
    gain_attn = gain_low_attn.astype(jnp.float32)
    gain_mlp = gain_low_mlp.astype(jnp.float32)
    inputs = tokens.astype(jnp.float32).reshape(flat_rows, breadth)
    normed = norm_rows(inputs, gain_attn).astype(jnp.bfloat16)
    projected = jnp.dot(normed, w_qkv, preferred_element_type=jnp.float32).reshape(
        seq_count, local_rows, 3 * breadth
    )
    offset_rows = lax.axis_index("ctx") * local_rows
    cosine, sine_table = turn_tables(offset_rows, local_rows, head_size)
    queries = rotate(split_heads(projected[..., :breadth], head_count), cosine, sine_table).astype(
        jnp.bfloat16
    )
    keys_own = (
        rotate(split_heads(projected[..., breadth : 2 * breadth], head_count), cosine, sine_table)
        .astype(jnp.bfloat16)
        .reshape(seq_count, local_rows, breadth)
    )
    values_own = projected[..., 2 * breadth :].astype(jnp.bfloat16)
    summed = jnp.zeros((seq_count, head_count, local_rows, head_size), jnp.float32)
    summit = jnp.full((seq_count, head_count, local_rows), -jnp.inf, jnp.float32)
    totals = jnp.zeros((seq_count, head_count, local_rows), jnp.float32)
    keys_in = lax.all_gather(keys_own, "ctx", axis=1, tiled=True)
    values_in = lax.all_gather(values_own, "ctx", axis=1, tiled=True)
    scores = (
        jnp.einsum(
            "sqhd,skhd->shqk",
            queries,
            split_heads(keys_in, head_count),
            preferred_element_type=jnp.float32,
        )
        * factor
    )
    raised = jnp.max(scores, axis=-1)
    shrink = jnp.exp(summit - raised)
    chances = jnp.exp(scores - raised[..., None])
    totals = totals * shrink + jnp.sum(chances, axis=-1)
    summed = summed * shrink[..., None] + jnp.einsum(
        "shqk,skhd->shqd",
        chances.astype(jnp.bfloat16),
        split_heads(values_in, head_count),
        preferred_element_type=jnp.float32,
    )
    summed, summit, totals = (summed, raised, totals)
    attended = (
        (summed / totals[..., None]).transpose(0, 2, 1, 3).reshape(seq_count, local_rows, breadth)
    )
    log_totals = summit + jnp.log(totals)
    attended_low = attended.astype(jnp.bfloat16).reshape(flat_rows, breadth)
    branch = jnp.dot(attended_low, w_attn, preferred_element_type=jnp.float32)
    middle = inputs + branch
    normed_mlp = norm_rows(middle, gain_mlp).astype(jnp.bfloat16)
    widened = jnp.dot(normed_mlp, w_inner, preferred_element_type=jnp.float32)
    gated_units = glu_units(widened).astype(jnp.bfloat16)
    output = (
        (middle + jnp.dot(gated_units, w_outer, preferred_element_type=jnp.float32))
        .astype(jnp.bfloat16)
        .reshape(seq_count, local_rows, breadth)
    )
    again = (
        lax.all_gather(shards[0], ("ctx", "dp"), axis=0, tiled=True),
        lax.all_gather(shards[1], ("ctx", "dp"), axis=0, tiled=True),
        lax.all_gather(shards[2], ("ctx", "dp"), axis=0, tiled=True),
        lax.all_gather(shards[3], ("ctx", "dp"), axis=1, tiled=True),
        lax.all_gather(shards[4], ("ctx", "dp"), axis=0, tiled=True),
        lax.all_gather(shards[5], ("ctx", "dp"), axis=0, tiled=True),
    )
    back_qkv, back_attn, back_inner, back_outer, back_gain_attn, back_gain_mlp = again
    gain_attn_back = back_gain_attn.astype(jnp.float32)
    gain_mlp_back = back_gain_mlp.astype(jnp.float32)
    grad_out = cotangent.astype(jnp.float32).reshape(flat_rows, breadth)
    grad_low = grad_out.astype(jnp.bfloat16)
    grad_outer = jnp.einsum("mf,md->fd", gated_units, grad_low, preferred_element_type=jnp.float32)
    grad_gated = jnp.einsum("md,fd->mf", grad_low, back_outer, preferred_element_type=jnp.float32)
    unused, glu_pull = jax.vjp(glu_units, widened)
    grad_wide = glu_pull(grad_gated)[0].astype(jnp.bfloat16)
    grad_inner = jnp.einsum("md,mf->df", normed_mlp, grad_wide, preferred_element_type=jnp.float32)
    grad_normed = jnp.einsum("mf,df->md", grad_wide, back_inner, preferred_element_type=jnp.float32)
    unused, norm_pull = jax.vjp(norm_rows, middle, gain_mlp_back)
    grad_middle, grad_gain_mlp = norm_pull(grad_normed)
    grad_middle = grad_middle + grad_out
    grad_branch = grad_middle.astype(jnp.bfloat16)
    grad_attn = jnp.einsum(
        "md,me->de", attended_low, grad_branch, preferred_element_type=jnp.float32
    )
    grad_mixed = (
        jnp.einsum("me,de->md", grad_branch, back_attn, preferred_element_type=jnp.float32)
        .astype(jnp.bfloat16)
        .reshape(seq_count, local_rows, breadth)
    )
    grad_heads = split_heads(grad_mixed, head_count)
    delta_rows = jnp.sum(
        grad_heads.astype(jnp.float32) * split_heads(attended, head_count), axis=-1
    ).transpose(0, 2, 1)
    stats_all = (
        lax.all_gather(log_totals, "ctx", axis=2, tiled=True),
        lax.all_gather(delta_rows, "ctx", axis=2, tiled=True),
    )
    keys_heads = split_heads(keys_own, head_count)
    values_heads = split_heads(values_own, head_count)
    zero_heads = jnp.zeros((seq_count, local_rows, head_count, head_size), jnp.float32)
    query_in = lax.all_gather(
        queries.reshape(seq_count, local_rows, breadth), "ctx", axis=1, tiled=True
    )
    grad_in = lax.all_gather(grad_mixed, "ctx", axis=1, tiled=True)
    query_heads = split_heads(query_in, head_count)
    grad_heads_in = split_heads(grad_in, head_count)
    lse_part = stats_all[0]
    delta_part = stats_all[1]
    scores = (
        jnp.einsum("sqhd,skhd->shqk", query_heads, keys_heads, preferred_element_type=jnp.float32)
        * factor
    )
    chances = jnp.exp(scores - lse_part[..., None])
    grad_values = jnp.einsum(
        "shqk,sqhd->skhd",
        chances.astype(jnp.bfloat16),
        grad_heads_in,
        preferred_element_type=jnp.float32,
    )
    grad_chances = jnp.einsum(
        "sqhd,skhd->shqk", grad_heads_in, values_heads, preferred_element_type=jnp.float32
    )
    grad_scores = (chances * (grad_chances - delta_part[..., None])).astype(jnp.bfloat16)
    grad_keys = (
        jnp.einsum("shqk,sqhd->skhd", grad_scores, query_heads, preferred_element_type=jnp.float32)
        * factor
    )
    grad_keys, grad_values = (grad_keys, grad_values)
    keys_in = lax.all_gather(keys_own, "ctx", axis=1, tiled=True)
    values_in = lax.all_gather(values_own, "ctx", axis=1, tiled=True)
    key_heads_in = split_heads(keys_in, head_count)
    scores = (
        jnp.einsum("sqhd,skhd->shqk", queries, key_heads_in, preferred_element_type=jnp.float32)
        * factor
    )
    chances = jnp.exp(scores - log_totals[..., None])
    grad_chances = jnp.einsum(
        "sqhd,skhd->shqk",
        grad_heads,
        split_heads(values_in, head_count),
        preferred_element_type=jnp.float32,
    )
    grad_scores = (chances * (grad_chances - delta_rows[..., None])).astype(jnp.bfloat16)
    grad_queries = (
        jnp.einsum("shqk,skhd->sqhd", grad_scores, key_heads_in, preferred_element_type=jnp.float32)
        * factor
    )

    def turn_only(values):
        return rotate(values, cosine, sine_table)

    unused, turn_pull = jax.vjp(turn_only, zero_heads)
    grad_query_pre = turn_pull(grad_queries)[0].reshape(flat_rows, breadth)
    grad_key_pre = turn_pull(grad_keys)[0].reshape(flat_rows, breadth)
    grad_proj = jnp.concatenate(
        [grad_query_pre, grad_key_pre, grad_values.reshape(flat_rows, breadth)], axis=-1
    ).astype(jnp.bfloat16)
    grad_qkv = jnp.einsum("md,me->de", normed, grad_proj, preferred_element_type=jnp.float32)
    grad_normed_attn = jnp.einsum(
        "me,de->md", grad_proj, back_qkv, preferred_element_type=jnp.float32
    )
    unused, first_pull = jax.vjp(norm_rows, inputs, gain_attn_back)
    grad_inputs, grad_gain_attn = first_pull(grad_normed_attn)
    tokens_grad = (
        (grad_middle + grad_inputs).astype(jnp.bfloat16).reshape(seq_count, local_rows, breadth)
    )
    summed_grads = (
        lax.psum_scatter(grad_qkv, ("ctx", "dp"), scatter_dimension=0, tiled=True),
        lax.psum_scatter(grad_attn, ("ctx", "dp"), scatter_dimension=0, tiled=True),
        lax.psum_scatter(grad_inner, ("ctx", "dp"), scatter_dimension=0, tiled=True),
        lax.psum_scatter(grad_outer, ("ctx", "dp"), scatter_dimension=1, tiled=True),
        lax.psum_scatter(grad_gain_attn, ("ctx", "dp"), scatter_dimension=0, tiled=True),
        lax.psum_scatter(grad_gain_mlp, ("ctx", "dp"), scatter_dimension=0, tiled=True),
    )
    return (
        output,
        tokens_grad,
        summed_grads[0],
        summed_grads[1],
        summed_grads[2],
        summed_grads[3],
        summed_grads[4],
        summed_grads[5],
    )


BF = jnp.bfloat16
F32 = jnp.float32
MESH_ID = pl.DeviceIdType.MESH
CHIPS = 4
PLANES = 4
SHARD = 24
BLOCK = 128
HALF = 512
WIDTH = 768
WQ_COLS = 640
WF_COLS = 896
WF_IN = 640
WF_OUT = 384
QO_COLS = 768
ISQRT2 = 0.7071067811865476
ISQRT2PI = 0.3989422804014327


def nn(a, b):
    return jnp.dot(a, b, preferred_element_type=F32)


def nt(a, b):
    return lax.dot_general(a, b, (((1,), (1,)), ((), ())), preferred_element_type=F32)


def lane_of(shape):
    return lax.broadcasted_iota(jnp.int32, shape, len(shape) - 1)


def shift(tile, amount):
    amount = amount % 128
    return tile if amount == 0 else pltpu.roll(tile, amount, 1)


def low(values):
    return values.astype(BF).astype(F32)


def standardize(values):
    center = values - jnp.mean(values, axis=-1, keepdims=True)
    spread = jnp.mean(center * center, axis=-1, keepdims=True)
    inverse = lax.rsqrt(spread + eps_norm)
    return center * inverse, inverse


def standardize_back(grad, unit, inverse):
    return inverse * (
        grad
        - jnp.mean(grad, axis=-1, keepdims=True)
        - unit * jnp.mean(grad * unit, axis=-1, keepdims=True)
    )


def tile(values, n):
    return values[:, 128 * n : 128 * (n + 1)]


def pair_low(a, b):
    return jnp.where(lane_of(a.shape) < 64, a, shift(b, 64))


def pair_high(a, b):
    return jnp.where(lane_of(a.shape) < 64, shift(a, 64), b)


def row_to_col(row):
    n = row.shape[1]
    same = lax.broadcasted_iota(jnp.int32, (n, n), 0) == lane_of((n, n))
    return jnp.sum(jnp.where(same, jnp.broadcast_to(row, (n, n)), 0.0), axis=1, keepdims=True)


def col_to_row(col):
    n = col.shape[0]
    same = lax.broadcasted_iota(jnp.int32, (n, n), 0) == lane_of((n, n))
    return jnp.sum(jnp.where(same, jnp.broadcast_to(col, (n, n)), 0.0), axis=0, keepdims=True)


SCRATCH = dict(
    sq=((CHIPS, SHARD, WQ_COLS), BF),
    so=((SHARD, WIDTH), BF),
    sf=((CHIPS, SHARD, WF_COLS), BF),
    wq=((WIDTH, WQ_COLS), BF),
    wo=((WIDTH, WIDTH), BF),
    wf=((WIDTH, WF_COLS), BF),
    xa=((2, HALF, WIDTH), BF),
    xh=((2, HALF, WIDTH), BF),
    xht=((WIDTH, HALF), BF),
    gb=((HALF, WIDTH), BF),
    gbt=((WIDTH, HALF), BF),
    kh=((3, 2 * HALF, 64), BF),
    vh=((3, 2 * HALF, 64), BF),
    kt=((3, 64, 2 * HALF), BF),
    vt=((3, 64, 2 * HALF), BF),
    qh=((3, HALF, 64), BF),
    et=((3, 2, 2 * HALF, 256), BF),
    ot=((256, HALF), F32),
    inv=((3, 2, 1, 256), F32),
    om=((CHIPS, HALF, 128), BF),
    on=((CHIPS, 256, 128), BF),
    o=((HALF, WIDTH), BF),
    oT=((WIDTH, HALF), BF),
    x2=((HALF, WIDTH), F32),
    n2=((HALF, WIDTH), BF),
    n2t=((WIDTH, HALF), BF),
    z=((HALF, WF_OUT), BF),
    du=((HALF, WF_IN), BF),
    dac=((HALF, 256), BF),
    outp=((HALF, WIDTH), BF),
    outr=((CHIPS, BLOCK, WIDTH), BF),
    dnp=((HALF, WIDTH), BF),
    dnr=((CHIPS, BLOCK, WIDTH), BF),
    dx2=((BLOCK, WIDTH), F32),
    m1=((CHIPS, BLOCK, 256), BF),
    m2=((CHIPS, BLOCK, 128), BF),
    dm1=((HALF, 256), BF),
    dm2=((HALF, 128), BF),
    dot=((192, HALF), F32),
    dqt=((256, HALF), F32),
    dkv=((3, HALF, 128), F32),
    dkvs=((3, HALF, 128), BF),
    dkvr=((3, HALF, 128), BF),
    dqkv=((HALF, WQ_COLS), BF),
    dxp=((HALF, WIDTH), BF),
    dxr=((CHIPS, BLOCK, WIDTH), BF),
)
for _name, _cols in (("f", WF_COLS), ("q", QO_COLS)):
    SCRATCH["g" + _name + "_part"] = ((WIDTH, _cols), BF)
    SCRATCH["g" + _name + "_core"] = ((CHIPS, 96, _cols), BF)
    SCRATCH["g" + _name + "_send"] = ((PLANES, CHIPS * SHARD, _cols), BF)
SCRATCH["gf_line"] = ((PLANES, CHIPS * SHARD, WF_COLS), BF)
SCRATCH["gf_sum"] = ((CHIPS, SHARD, WF_COLS), BF)
SCRATCH["gf_all"] = ((CHIPS, SHARD, WF_COLS), BF)
SCRATCH["gq_all"] = ((CHIPS * PLANES, SHARD, QO_COLS), BF)
N_SEM = 240


def layer_kernel(*refs):
    ins, outs = refs[:9], refs[9:17]
    x_ref, g_ref, wq_ref, wo_ref, wi_ref, wu_ref, ga_ref, gm_ref, trig = ins
    out_ref, tg_ref, gq_ref, go_ref, gi_ref, gu_ref, gga_ref, ggm_ref = outs
    s = dict(zip(SCRATCH, refs[17 : 17 + len(SCRATCH)]))
    send_sem, recv_sem = refs[17 + len(SCRATCH) :]

    i = lax.axis_index("ctx")
    p = lax.axis_index("dp")
    c = lax.div(i, 2)
    h = lax.rem(i, 2)
    other = 1 - h

    def chip(k):
        return lax.rem(c + k, CHIPS)

    def plane(k):
        return lax.rem(p + k, PLANES)

    def dev(kc, kp):
        return (2 * chip(kc) + h, plane(kp))

    partner = (2 * c + other, p)
    used = [0]
    pending = []

    def sems(n):
        used[0] += n
        assert used[0] <= N_SEM
        return used[0] - n

    def copy(src, dst, sem, device):
        return pltpu.make_async_remote_copy(
            src_ref=src,
            dst_ref=dst,
            send_sem=send_sem.at[sem],
            recv_sem=recv_sem.at[sem],
            device_id=device,
            device_id_type=MESH_ID,
        )

    def start(src, dst, sem, device):
        made = copy(src, dst, sem, device)
        made.start()
        pending.append(made)
        return made

    def rows(k, n=BLOCK):
        return pl.ds(pl.multiple_of(k * n, 8), n)

    far = [(kc, kp) for kc in (0, 1, 2, 3) for kp in (2, 3, 1, 0) if (kc, kp) != (0, 0)]

    barrier = pltpu.get_barrier_semaphore()
    for kc, kp in far:
        pl.semaphore_signal(barrier, inc=1, device_id=dev(kc, kp), device_id_type=MESH_ID)
    pl.semaphore_signal(barrier, inc=1, device_id=partner, device_id_type=MESH_ID)

    lane = lane_of((SHARD, 128))
    gain_a = low(row_to_col(ga_ref[...]))
    gain_m = low(row_to_col(gm_ref[...]))

    def scaled(ref, n, gain):
        return low(ref[:, 128 * n : 128 * (n + 1)]) * gain

    for j in range(CHIPS):
        m = 4 + j // 2
        pair = pair_low if j % 2 == 0 else pair_high
        q2, k2, v2 = (scaled(wq_ref, 6 * part + m, gain_a) for part in range(3))
        s["sq"][j, :, 0:128] = scaled(wq_ref, 6 + j, gain_a).astype(BF)
        s["sq"][j, :, 128:256] = scaled(wq_ref, 12 + j, gain_a).astype(BF)
        s["sq"][j, :, 256:384] = pair(k2, v2).astype(BF)
        s["sq"][j, :, 384:512] = scaled(wq_ref, j, gain_a).astype(BF)
        s["sq"][j, :, 512:640] = pair(q2, jnp.zeros_like(q2)).astype(BF)
    pl.semaphore_wait(barrier, len(far) + 1)

    def here(n):
        return pl.ds(pl.multiple_of((2 * n + h) * 96 + p * SHARD, 8), SHARD)

    def spread(made, dst, base):
        for one in made:
            one.wait_recv()
        passed = []
        for n in range(CHIPS):
            part = dst.at[rows(2 * n + h, 96)]
            passed.append(start(part, part, base + n, partner))
        return passed

    q_base = sems(len(far) + CHIPS)
    q_made = [
        start(s["sq"].at[chip(kc)], s["wq"].at[here(c)], q_base + n, dev(kc, kp))
        for n, (kc, kp) in enumerate(far)
    ]
    x_base = sems(8)
    x_made = [
        start(x_ref, s["xa"].at[0, rows(c)], x_base + k, dev(k, 0)) for k in (2, 1, 3)
    ]
    x_core = [start(x_ref, s["xa"].at[1, rows(c)], x_base + 4, partner)]
    s["wq"][here(c), :] = s["sq"][c]
    s["xa"][0, rows(c), :] = x_ref[...]

    for j in range(CHIPS):
        s["sf"][j, :, 0:128] = scaled(wi_ref, 2 * j, gain_m).astype(BF)
        s["sf"][j, :, 128:256] = scaled(wi_ref, 2 * j + 1, gain_m).astype(BF)
        s["sf"][j, :, 256:384] = scaled(wi_ref, 9 + 2 * j, gain_m).astype(BF)
        s["sf"][j, :, 384:512] = scaled(wi_ref, 10 + 2 * j, gain_m).astype(BF)
        a8, g8 = scaled(wi_ref, 8, gain_m), scaled(wi_ref, 17, gain_m)
        mix = jnp.where(lane < 32, shift(a8, -32 * j), shift(g8, 32 - 32 * j))
        u8 = jnp.where(lane < 96, shift(wu_ref[:, 1024:1152], 64 - 32 * j), 0.0)
        s["sf"][j, :, 512:640] = jnp.where(lane < 64, mix, u8).astype(BF)
        s["sf"][j, :, 640:896] = wu_ref[:, 256 * j : 256 * j + 256].astype(BF)
    f_base = sems(6 * CHIPS)
    f_made = [
        start(s["sf"].at[chip(k)], s["wf"].at[here(c)], f_base + k, dev(k, 0)) for k in (2, 1, 3)
    ]
    s["wf"][here(c), :] = s["sf"][c]
    s["so"][...] = wo_ref[...].astype(BF)
    s["wo"][here(c), :] = s["so"][...]
    s["gb"][rows(c), :] = g_ref[...]

    def unit_block(part, k):
        unit, unused = standardize(s["xa"][part, rows(k), :].astype(F32))
        s["xh"][part, rows(k), :] = unit.astype(BF)
        if part == 0:
            s["xht"][:, rows(k)] = unit.T.astype(BF)

    unit_block(0, c)
    for n, k in enumerate((2, 1, 3)):
        x_made[n].wait_recv()
        block = rows(lax.rem(c + CHIPS - k, CHIPS))
        x_core.append(start(s["xa"].at[0, block], s["xa"].at[1, block], x_base + 4 + k, partner))
        unit_block(0, lax.rem(c + CHIPS - k, CHIPS))
    for one in x_core:
        one.wait_recv()

    def unit_other(k, carry):
        unit_block(1, k)
        return carry

    lax.fori_loop(0, CHIPS, unit_other, 0)

    for one in q_made:
        one.wait_send()
    pending[:] = [one for one in pending if all(one is not sent for sent in q_made)]
    o_base = sems(12)
    o_line = [
        start(s["so"], s["wo"].at[here(c)], o_base + k, dev(0, k)) for k in (2, 1, 3)
    ]
    for one in f_made:
        one.wait_recv()
    f_line = [
        start(s["wf"].at[here(n)], s["wf"].at[here(n)], f_base + 4 * (k + 1) + n, dev(0, k))
        for k in (2, 1, 3)
        for n in range(CHIPS)
    ]
    q_passed = spread(q_made, s["wq"], q_base + len(far))
    g_base = sems(4)
    g_made = [start(g_ref, s["gb"].at[rows(c)], g_base + k, dev(k, 0)) for k in (2, 1, 3)]

    def turn(k, half):
        cb, sb = trig[pl.ds(256 + k, 1), :], trig[pl.ds(264 + k, 1), :]
        cr, sr = trig[0:128, :], trig[128:256, :]
        cos, sin = cr * cb - sr * sb, sr * cb + cr * sb
        if half:
            first = lane_of(cos.shape) < 64
            cos, sin = jnp.where(first, cos, 1.0), jnp.where(first, sin, 0.0)
        return cos, sin

    def swap(t):
        inner = lax.rem(lane_of(t.shape), 64) < 32
        return jnp.where(inner, shift(t, 96), shift(t, 32))

    def turned(t, table):
        return t * table[0] + swap(t) * table[1]

    def turned_back(t, table):
        return t * table[0] - swap(t) * table[1]

    def table_pair(b, parity, half):
        first, second = turn(4 * b + parity, half), turn(4 * b + 2 + parity, half)
        return tuple(jnp.concatenate(both, axis=0) for both in zip(first, second))

    for one in q_passed:
        one.wait_recv()

    def high(t):
        return shift(t, 64)[:, :64]

    def project(part, parity):
        def step(b, carry):
            block = pl.ds(pl.multiple_of(b * 256, 256), 256)
            there = pl.ds(pl.multiple_of(part * HALF + b * 256, 256), 256)
            full, half = table_pair(b, parity, False), table_pair(b, parity, True)
            cols = WQ_COLS if part == 0 else 384
            y = nn(s["xh"][part, block, :], s["wq"][:, :cols])
            k01 = turned(tile(y, 0), full)
            v01 = tile(y, 1)
            kv2 = turned(tile(y, 2), half)
            s["kh"][0, there, :] = k01[:, :64].astype(BF)
            s["kh"][1, there, :] = high(k01).astype(BF)
            s["kh"][2, there, :] = kv2[:, :64].astype(BF)
            s["vh"][0, there, :] = v01[:, :64].astype(BF)
            s["vh"][1, there, :] = high(v01).astype(BF)
            s["vh"][2, there, :] = high(kv2).astype(BF)
            kt, vt, mt = k01.T.astype(BF), v01.T.astype(BF), kv2.T.astype(BF)
            s["kt"][0, :, there] = kt[:64]
            s["kt"][1, :, there] = kt[64:]
            s["kt"][2, :, there] = mt[:64]
            s["vt"][0, :, there] = vt[:64]
            s["vt"][1, :, there] = vt[64:]
            s["vt"][2, :, there] = mt[64:]
            if part == 0:
                q01 = turned(tile(y, 3), full) * 0.125
                q2 = turned(tile(y, 4), half) * 0.125
                s["qh"][0, block, :] = q01[:, :64].astype(BF)
                s["qh"][1, block, :] = high(q01).astype(BF)
                s["qh"][2, block, :] = q2[:, :64].astype(BF)
            return carry

        lax.fori_loop(0, 2, step, 0)

    project(0, h)
    project(1, other)

    for one in o_line:
        one.wait_recv()
    o_mine = s["wo"].at[rows(i, 96)]
    o_made = [start(o_mine, o_mine, o_base + 3 + k, dev(k, 0)) for k in (2, 1, 3)]
    o_core = [start(o_mine, o_mine, o_base + 7, partner)]

    def attend(t, carry):
        hd, b = lax.div(t, 2), lax.rem(t, 2)
        block = pl.ds(pl.multiple_of(b * 256, 256), 256)
        scores = nt(s["kh"][hd], s["qh"][hd, block, :])
        raised = jnp.exp(scores - jnp.max(scores, axis=0, keepdims=True))
        inverse = 1.0 / jnp.sum(raised, axis=0, keepdims=True)
        packed = raised.astype(BF)
        s["et"][hd, b] = packed
        s["inv"][hd, b] = inverse
        s["ot"][pl.ds(pl.multiple_of(hd * 64, 64), 64), block] = nn(s["vt"][hd], packed) * inverse
        return carry

    lax.fori_loop(0, 4, attend, 0)
    om_base = sems(8)
    s["om"][c] = s["ot"][0:128, :].T.astype(BF)
    om_made = [
        start(s["om"].at[c], s["om"].at[c], om_base + k, dev(k, 0)) for k in (2, 1, 3)
    ]
    lax.fori_loop(4, 6, attend, 0)
    last = jnp.concatenate([s["ot"][128:192, 0:256], s["ot"][128:192, 256:512]], axis=0)
    s["on"][c] = last.T.astype(BF)
    om_made += [
        start(s["on"].at[c], s["on"].at[c], om_base + 4 + k, dev(k, 0)) for k in (2, 1, 3)
    ]

    for n, k in enumerate((2, 1, 3)):
        o_made[n].wait_recv()
        block = s["wo"].at[rows(2 * lax.rem(c + CHIPS - k, CHIPS) + h, 96)]
        o_core.append(start(block, block, o_base + 7 + k, partner))
    for one in g_made:
        one.wait_recv()

    def flip_grad(k, carry):
        s["gbt"][:, rows(k)] = s["gb"][rows(k), :].astype(F32).T.astype(BF)
        return carry

    lax.fori_loop(0, CHIPS, flip_grad, 0)
    f_passed = spread(f_line, s["wf"], f_base + 4)
    for one in o_core + f_passed:
        one.wait_recv()
    for one in om_made:
        one.wait_recv()
    for j in range(CHIPS):
        s["o"][:, 128 * j : 128 * (j + 1)] = s["om"][j]
    for m in range(2):
        first, second = s["on"][2 * m].astype(F32), s["on"][2 * m + 1].astype(F32)
        s["o"][0:256, 128 * (4 + m) : 128 * (5 + m)] = pair_low(first, second).astype(BF)
        s["o"][256:512, 128 * (4 + m) : 128 * (5 + m)] = pair_high(first, second).astype(BF)

    dn_base = sems(4)

    def feed(k, carry):
        t = chip(k)
        block = rows(t)
        x2 = s["xa"][0, block, :].astype(F32) + nn(s["o"][block, :], s["wo"][...])
        s["x2"][block, :] = x2
        unit, unused = standardize(x2)
        unit_low = unit.astype(BF)
        s["n2"][block, :] = unit_low
        u = nn(unit_low, s["wf"][:, 0:WF_IN])
        dz = nn(s["gb"][block, :], s["wf"][:, 512:WF_COLS])

        def gate(a, g, dz_part):
            share = 0.5 + 0.5 * lax.erf(a * ISQRT2)
            bell = a * ISQRT2PI * jnp.exp(-0.5 * a * a)
            z_part = a * share * g
            da = dz_part * g * (share + bell)
            return z_part, da, dz_part * a * share

        z01, da01, dg01 = gate(u[:, 0:256], u[:, 256:512], dz[:, 128:384])
        along = lane_of((BLOCK, 128))
        mix = jnp.where(along < 64, u[:, 512:640], 0.0)
        dz2 = jnp.where(along < 32, shift(dz[:, 0:128], 64), 0.0)
        z2, da2, dg2 = gate(mix, shift(mix, 96), dz2)
        s["z"][block, 0:128] = shift(z2, 64).astype(BF)
        s["z"][block, 128:384] = z01.astype(BF)
        s["du"][block, 0:256] = da01.astype(BF)
        s["du"][block, 256:512] = dg01.astype(BF)
        s["du"][block, 512:640] = (da2 + shift(dg2, 32)).astype(BF)
        s["dnp"][block, :] = nt(s["du"][block, :], s["wf"][:, 0:WF_IN]).astype(BF)

        @pl.when(k < CHIPS)
        def _():
            copy(s["dnp"].at[block], s["dnr"].at[c], dn_base + k - 1, dev(k, 0)).start()

        return carry

    lax.fori_loop(1, CHIPS + 1, feed, 0)
    dn_made = [
        copy(s["dnp"].at[rows(chip(k))], s["dnr"].at[c], dn_base + k - 1, dev(k, 0)) for k in (1, 2, 3)
    ]
    pending.extend(dn_made)

    def exchange(name):
        part, core = s["g" + name + "_part"], s["g" + name + "_core"]
        base = sems(CHIPS)
        return [
            start(part.at[rows(2 * n + other, 96)], core.at[n], base + n, partner)
            for n in range(CHIPS)
        ]

    def merge(name, made):
        part, core = s["g" + name + "_part"], s["g" + name + "_core"]
        for one in made:
            one.wait_recv()
        for n in range(CHIPS):
            both = (part[rows(2 * n + h, 96), :].astype(F32) + core[n].astype(F32)).astype(BF)
            for q in range(PLANES):
                s["g" + name + "_send"][q, SHARD * n : SHARD * (n + 1), :] = both[
                    SHARD * q : SHARD * (q + 1)
                ]

    thirds = [slice(256 * b, 256 * (b + 1)) for b in range(3)]

    def flip_unit(k, carry):
        s["n2t"][:, rows(k)] = s["n2"][rows(k), :].astype(F32).T.astype(BF)
        s["oT"][:, rows(k)] = s["o"][rows(k), :].astype(F32).T.astype(BF)
        return carry

    lax.fori_loop(0, CHIPS, flip_unit, 0)
    for third in thirds:
        wide = nn(s["n2t"][third, :], s["du"][...])
        tall = nn(s["gbt"][third, :], s["z"][...])
        s["gf_part"][third, 0:512] = wide[:, 0:512].astype(BF)
        s["gf_part"][third, 512:640] = (wide[:, 512:640] + tall[:, 0:128]).astype(BF)
        s["gf_part"][third, 640:896] = tall[:, 128:384].astype(BF)
    f_core = exchange("f")

    for one in dn_made:
        one.wait_recv()
    grad = s["dnp"][rows(c), :].astype(F32)
    for k in (1, 2, 3):
        grad = grad + s["dnr"][chip(k)].astype(F32)
    unit2, inverse2 = standardize(s["x2"][rows(c), :])
    dx2 = g_ref[...].astype(F32) + standardize_back(grad, unit2, inverse2)
    s["dx2"][...] = dx2
    da = dx2.astype(BF)
    do = nt(da, s["wo"][...])
    da = da.astype(F32)
    for j in range(CHIPS):
        m = 4 + j // 2
        pair = pair_low if j % 2 == 0 else pair_high
        s["m1"][j, :, 0:128] = tile(do, j).astype(BF)
        s["m1"][j, :, 128:256] = pair(tile(do, m), tile(da, m)).astype(BF)
        s["m2"][j] = tile(da, j).astype(BF)
    m_base = sems(8)
    m1_made = [
        start(s["m1"].at[chip(k)], s["dm1"].at[rows(c)], m_base + k, dev(k, 0)) for k in (2, 1, 3)
    ]
    m2_made = [
        start(s["m2"].at[chip(k)], s["dm2"].at[rows(c)], m_base + 4 + k, dev(k, 0))
        for k in (2, 1, 3)
    ]
    s["dm1"][rows(c), :] = s["m1"][c]
    s["dm2"][rows(c), :] = s["m2"][c]
    merge("f", f_core)
    f_base = sems(8)
    f_line = [
        start(s["gf_send"].at[plane(k)], s["gf_line"].at[p], f_base + k, dev(0, k)) for k in (2, 1, 3)
    ]
    s["gf_line"][p] = s["gf_send"][p]

    out_base = sems(4)

    def project_out(k, carry):
        block = rows(chip(k))
        s["outp"][block, :] = nt(s["z"][block, :], s["wf"][:, 512:WF_COLS]).astype(BF)

        @pl.when(k < CHIPS)
        def _():
            copy(s["outp"].at[block], s["outr"].at[c], out_base + k - 1, dev(k, 0)).start()

        return carry

    lax.fori_loop(1, CHIPS + 1, project_out, 0)
    out_made = [
        copy(s["outp"].at[rows(chip(k))], s["outr"].at[c], out_base + k - 1, dev(k, 0)) for k in (1, 2, 3)
    ]
    pending.extend(out_made)


    for one in m1_made:
        one.wait_recv()

    s["dot"][0:128, :] = s["dm1"][:, 0:128].astype(F32).T
    s["dot"][128:192, :] = s["dm1"][:, 128:256].astype(F32).T[:64]
    s["dqt"][192:256, :] = jnp.zeros((64, HALF), F32)

    def attend_back(hd, carry):
        dk = jnp.zeros((2 * HALF, 64), F32)
        dv = jnp.zeros((2 * HALF, 64), F32)
        head = pl.ds(pl.multiple_of(hd * 64, 64), 64)
        for b in range(2):
            block = slice(256 * b, 256 * (b + 1))
            do_t = s["dot"][head, block] * s["inv"][hd, b]
            delta = jnp.sum(do_t * s["ot"][head, block], axis=0, keepdims=True)
            dp = nn(s["vh"][hd], do_t.astype(BF))
            packed = s["et"][hd, b]
            ds = (packed.astype(F32) * (dp - delta)).astype(BF)
            s["dqt"][head, block] = nn(s["kt"][hd], ds) * 0.125
            dv = dv + nn(packed, do_t.T.astype(BF))
            dk = dk + nn(ds, s["qh"][hd, block, :])
        both = jnp.concatenate([dk, dv], axis=1)
        s["dkv"][hd] = both[:HALF]
        s["dkvs"][hd] = both[HALF:].astype(BF)
        return carry

    lax.fori_loop(0, 3, attend_back, 0)
    dkv_made = start(s["dkvs"], s["dkvr"], sems(1), partner)
    dq = s["dqt"][...].T
    dkv_made.wait_recv()
    for b in range(CHIPS):
        block = slice(128 * b, 128 * (b + 1))
        full, half = turn(2 * b + h, False), turn(2 * b + h, True)
        one, two, three = (
            s["dkv"][hd, block, :] + s["dkvr"][hd, block, :].astype(F32) for hd in range(3)
        )
        s["dqkv"][block, 0:128] = turned_back(pair_low(one, two), full).astype(BF)
        s["dqkv"][block, 128:256] = pair_high(one, two).astype(BF)
        s["dqkv"][block, 256:384] = turned_back(three, half).astype(BF)
        s["dqkv"][block, 384:512] = turned_back(dq[block, 0:128], full).astype(BF)
        s["dqkv"][block, 512:640] = turned_back(dq[block, 128:256], half).astype(BF)

    dx_base = sems(4)

    def project_back(k, carry):
        block = rows(chip(k))
        s["dxp"][block, :] = nt(s["dqkv"][block, :], s["wq"][...]).astype(BF)

        @pl.when(k < CHIPS)
        def _():
            copy(s["dxp"].at[block], s["dxr"].at[c], dx_base + k - 1, dev(k, 0)).start()

        return carry

    lax.fori_loop(1, CHIPS + 1, project_back, 0)
    dx_made = [
        copy(s["dxp"].at[rows(chip(k))], s["dxr"].at[c], dx_base + k - 1, dev(k, 0)) for k in (1, 2, 3)
    ]
    pending.extend(dx_made)
    for one in m2_made:
        one.wait_recv()
    mixed = s["dm1"][:, 128:256].astype(F32)
    s["dac"][:, 0:128] = jnp.where(lane_of(mixed.shape) < 64, 0.0, mixed).astype(BF)
    s["dac"][:, 128:256] = s["dm2"][...]
    for third in thirds:
        wide = nn(s["xht"][third, :], s["dqkv"][...])
        tall = nn(s["oT"][third, :], s["dac"][...])
        s["gq_part"][third, 0:512] = wide[:, 0:512].astype(BF)
        s["gq_part"][third, 512:640] = (wide[:, 512:640] + tall[:, 0:128]).astype(BF)
        s["gq_part"][third, 640:768] = tall[:, 128:256].astype(BF)
    q_core = exchange("q")
    for one in f_line:
        one.wait_recv()
    for n in range(CHIPS):
        block = slice(SHARD * n, SHARD * (n + 1))
        total = s["gf_line"][0, block, :].astype(F32)
        for q in range(1, PLANES):
            total = total + s["gf_line"][q, block, :].astype(F32)
        s["gf_sum"][n] = total.astype(BF)
    f_all = [start(s["gf_sum"].at[chip(k)], s["gf_all"].at[c], f_base + 4 + k, dev(k, 0)) for k in (2, 1, 3)]
    s["gf_all"][c] = s["gf_sum"][c]
    merge("q", q_core)
    base = sems(len(far))
    mine = c * PLANES + p

    def cut(kc, kp):
        return s["gq_send"].at[plane(kp), rows(chip(kc), SHARD)]

    q_all = [
        start(cut(kc, kp), s["gq_all"].at[mine], base + n, dev(kc, kp))
        for n, (kc, kp) in enumerate(far)
    ]
    s["gq_all"][mine] = s["gq_send"][p, rows(c, SHARD), :]

    for one in out_made:
        one.wait_recv()
    total = s["x2"][rows(c), :] + s["outp"][rows(c), :].astype(F32)
    for k in (1, 2, 3):
        total = total + s["outr"][chip(k)].astype(F32)
    out_ref[...] = total.astype(BF)

    for one in f_all:
        one.wait_recv()
    f_sum = [s["gf_all"][j].astype(F32) for j in range(CHIPS)]

    def ninth(first):
        inside = (lane >= first) & (lane < first + 32)
        return sum(
            shift(jnp.where(inside, tile(f_sum[j], 4), 0.0), 32 * j - first) for j in range(CHIPS)
        )

    for j in range(8):
        gu_ref[:, 128 * j : 128 * (j + 1)] = tile(f_sum[j // 2], 5 + j % 2)
    gu_ref[:, 1024:1152] = ninth(64)
    tiles = [tile(f_sum[j // 2], j % 2) for j in range(8)] + [ninth(0)]
    tiles += [tile(f_sum[j // 2], 2 + j % 2) for j in range(8)] + [ninth(32)]

    def finish(tiles, gain, weight, grad_out, gain_out):
        along = jnp.zeros((SHARD, 128), F32)
        for n, one in enumerate(tiles):
            grad_out[:, 128 * n : 128 * (n + 1)] = one * gain
            along = along + one * low(weight[:, 128 * n : 128 * (n + 1)])
        gain_out[...] = col_to_row(jnp.sum(along, axis=1, keepdims=True))

    finish(tiles, gain_m, wi_ref, gi_ref, ggm_ref)

    for one in dx_made:
        one.wait_recv()
    grad = s["dxp"][rows(c), :].astype(F32)
    for k in (1, 2, 3):
        grad = grad + s["dxr"][chip(k)].astype(F32)
    unit1, inverse1 = standardize(x_ref[...].astype(F32))
    tg_ref[...] = (s["dx2"][...] + standardize_back(grad, unit1, inverse1)).astype(BF)

    for one in q_all:
        one.wait_recv()
    q_sum = [sum(s["gq_all"][PLANES * j + q].astype(F32) for q in range(PLANES)) for j in range(CHIPS)]
    tiles = [tile(q_sum[j], 3) for j in range(4)]
    tiles += [pair_low(tile(q_sum[2 * m], 4), tile(q_sum[2 * m + 1], 4)) for m in range(2)]
    tiles += [tile(q_sum[j], 0) for j in range(4)]
    tiles += [pair_low(tile(q_sum[2 * m], 2), tile(q_sum[2 * m + 1], 2)) for m in range(2)]
    tiles += [tile(q_sum[j], 1) for j in range(4)]
    tiles += [pair_high(tile(q_sum[2 * m], 2), tile(q_sum[2 * m + 1], 2)) for m in range(2)]
    finish(tiles, gain_a, wq_ref, gq_ref, gga_ref)

    for j in range(CHIPS):
        go_ref[:, 128 * j : 128 * (j + 1)] = tile(q_sum[j], 5)
    for m in range(2):
        go_ref[:, 128 * (4 + m) : 128 * (5 + m)] = pair_high(
            tile(q_sum[2 * m], 4), tile(q_sum[2 * m + 1], 4)
        )

    for one in pending:
        one.wait_send()


def deliver(*refs):
    for source, target in zip(refs[:8], refs[8:]):
        target[...] = source[...]


def trig_rows(head_size):
    lanes = np.arange(128)
    inverse = theta_base ** (-((lanes % (head_size // 2)) * 2.0 / head_size))
    sign = np.where(lanes % head_size < head_size // 2, -1.0, 1.0)
    near = np.arange(BLOCK)[:, None] * inverse[None, :]
    far = (np.arange(8) * BLOCK)[:, None] * inverse[None, :]
    parts = [np.cos(near), np.sin(near) * sign, np.cos(far), np.sin(far) * sign]
    return np.concatenate(parts, axis=0).astype(np.float32)


def fused_body(
    tokens, cotangent, qkv_weight, attn_out_weight, mlp_in_weight, mlp_out_weight, attn_gain, mlp_gain
):
    vmem = pl.BlockSpec(memory_space=pltpu.VMEM)
    operands = (
        tokens.reshape(BLOCK, WIDTH),
        cotangent.reshape(BLOCK, WIDTH),
        qkv_weight,
        attn_out_weight,
        mlp_in_weight,
        mlp_out_weight.T,
        attn_gain.reshape(1, SHARD),
        mlp_gain.reshape(1, SHARD),
        jnp.asarray(trig_rows(64)),
    )
    shapes = (
        ((BLOCK, WIDTH), BF),
        ((BLOCK, WIDTH), BF),
        (qkv_weight.shape, F32),
        (attn_out_weight.shape, F32),
        (mlp_in_weight.shape, F32),
        (mlp_out_weight.shape[::-1], F32),
        ((1, SHARD), F32),
        ((1, SHARD), F32),
    )
    results = pl.pallas_call(
        layer_kernel,
        out_shape=tuple(jax.ShapeDtypeStruct(*one) for one in shapes),
        in_specs=[vmem] * len(operands),
        out_specs=(vmem,) * len(shapes),
        scratch_shapes=[pltpu.VMEM(*one) for one in SCRATCH.values()]
        + [pltpu.SemaphoreType.DMA((N_SEM,)), pltpu.SemaphoreType.DMA((N_SEM,))],
        compiler_params=pltpu.CompilerParams(
            collective_id=0, has_side_effects=True, vmem_limit_bytes=64 * 1024 * 1024 - 131072
        ),
        name="attention_layer",
    )(*operands)
    results = pl.pallas_call(
        deliver,
        out_shape=tuple(jax.ShapeDtypeStruct(*one) for one in shapes),
        in_specs=[vmem] * len(shapes),
        out_specs=(vmem,) * len(shapes),
        name="deliver",
    )(*results)
    return (
        results[0].reshape(tokens.shape),
        results[1].reshape(tokens.shape),
        *results[2:5],
        results[5].T,
        results[6].reshape(SHARD),
        results[7].reshape(SHARD),
    )


def fits(mesh, tokens, qkv_weight):
    return (
        mesh.shape["ctx"] == 2 * CHIPS
        and mesh.shape["dp"] == PLANES
        and tokens.shape == (PLANES, 8 * BLOCK, WIDTH)
        and qkv_weight.shape == (WIDTH, 3 * WIDTH)
    )


def solution(mesh):

    def run(*arrays):
        tokens, qkv_weight = arrays[0], arrays[2]
        chosen = fused_body if fits(mesh, tokens, qkv_weight) else body
        return jax.shard_map(
            chosen,
            mesh=mesh,
            in_specs=placed,
            out_specs=placed,
            check_vma=False,
        )(*arrays)

    placed = (
        P("dp", "ctx", None),
        P("dp", "ctx", None),
        P(("ctx", "dp"), None),
        P(("ctx", "dp"), None),
        P(("ctx", "dp"), None),
        P(None, ("ctx", "dp")),
        P(("ctx", "dp")),
        P(("ctx", "dp")),
    )
    return run
```
